32 devices in a mesh: gx: 8 (over z, x), gy: 4 (over y, core).
Axes of the slice: x: 2, y: 2, z: 4, core: 2. Of those that a mesh axis runs over, the one named last changes fastest.
Arguments:
- parcel_props: float32 [16, 131072], P(None, ('gx', 'gy')), may hold values from -6 to 6
- size_class: int32 [131072], P(('gx', 'gy')), may hold values from 0 to 7
- dest_owner: int32 [131072, 1], P(('gx', 'gy')), may hold values from 0 to 31; in each aligned block of 4096 rows (0 to 4095, 4096 to 8191, ...) at most 512 rows name the same one
- dest_local: int32 [131072], P(('gx', 'gy')), may hold values from 0 to 4095
- class_table: float32 [8, 16], replicated, may hold values from 0.5 to 2
- gas_density: float32 [256, 512], P('gx', 'gy'), may hold values from 0.5 to 2
- gas_rest: float32 [4, 256, 512], P(None, 'gx', 'gy'), may hold values from -6 to 6
Outputs:
- new_density: float32 [256, 512], P('gx', 'gy')
- new_rest: float32 [4, 256, 512], P(None, 'gx', 'gy')
The draws below stay inside these ranges and needn't reach their ends.
Inputs may be any that keep to these rules, and one draw needn't show every extreme that they name: `dest_owner`: among the parcels of one device, no owner device is named by more than 512 of them, a bound that some block reaches.
All inputs are finite; a program needn't handle non-finite values.
Results may differ from the reference program's by a relative error of at most 0.00015.
Values sent between devices are 32-bit elements; how exact they have to be, the bound alone decides.
No kernel may reach another device: no remote copies, remote signals or barrier semaphores. Data moves between devices by JAX's collectives and lax.ppermute only.
A program may use at most 64 MiB of HBM per device.

```python
import math
import jax
import jax.numpy as jnp
import numpy as np
from jax import lax

PROPS = 16
CLASSES = 8
PARC_DEV = 4096
LX = 32
LY = 128
CAP = 512
PARCELS = 131072
NX = 256
NY = 512
N_GY = 4
DEVICES = 32


def place_ends(drawn, rng, least, high):
    longest = drawn.shape.index(max(drawn.shape))
    spots = []
    for shift in (0, 1):
        where = [jax.random.randint(jax.random.fold_in(rng, axis), (), 0, length) for axis, length in enumerate(drawn.shape)]
        where[longest] = (where[longest] + shift) % drawn.shape[longest]
        spots.append(tuple(where))
    return drawn.at[spots[0]].set(least).at[spots[1]].set(high)


def steps_of(own_key, shape, shards, least, largest):
    def one(axis_at, shards_of):
        heights = jax.random.uniform(jax.random.fold_in(jax.random.fold_in(own_key, 6), axis_at), (shards_of,), jnp.float32, least / len(shards), largest / len(shards))
        return jnp.repeat(jnp.exp(heights), shape[axis_at] // shards_of).reshape((-1,) + (1,) * (len(shape) - axis_at - 1))

    level = one(*shards[0])
    for cut in shards[1:]:
        level = level * one(*cut)
    return level


def routed_block(key, own, number, rows, count, top, limit, lean):
    sequence = jax.random.permutation(key, count)
    packed, common = load_shares(count, rows * top, limit, lean, True), load_shares(count, rows * top, limit, lean, False)
    places = jnp.arange(count)

    def named(tallies, rotation):
        used = int((tallies > 0).sum())
        fixed = max(1, used // 4)
        shifted = fixed + (places - fixed + rotation * (used - fixed)) % max(1, count - fixed)
        return jnp.zeros((count,), jnp.int32).at[sequence[jnp.where(places < fixed, places, shifted)]].set(jnp.asarray(tallies, jnp.int32))

    tallies = jnp.where(number % 4 == 0, named(packed, number // 4), named(common, number - number // 4 - 1))
    mixed = jax.random.permutation(jax.random.fold_in(own, 3), count)
    source_of, sink = mixed[0:count // 2 * 2:2], mixed[1:count // 2 * 2:2]
    margin = jnp.minimum(tallies[source_of] - 1, limit - tallies[sink]) // 2
    margin = jnp.where((source_of == sequence[0]) | (sink == sequence[0]) | (tallies[sink] == 0), 0, jnp.maximum(margin, 0))
    shifted = jax.random.randint(jax.random.fold_in(own, 4), (count // 2,), 0, 1 << 20) % (margin + 1)
    tallies = tallies.at[source_of].add(-shifted).at[sink].add(shifted)
    members = jnp.searchsorted(jnp.cumsum(tallies), jnp.arange(rows * top), side="right").astype(jnp.int32)
    table = members.reshape(top, rows).T
    table = table[jax.random.permutation(jax.random.fold_in(own, 1), rows)]
    rotation = jax.random.randint(jax.random.fold_in(own, 2), (rows, 1), 0, top)
    return jnp.take_along_axis(table, (jnp.arange(top)[None, :] + rotation) % top, axis=1)


def load_shares(count, total, most, lean, full):
    weights = [(1 << 20) // math.isqrt(standing ** lean) + 1 for standing in range(1, count + 1)]
    largest = most if full else min(most, max(-(-total // count), total * weights[0] // sum(weights)))
    least = 1 if total - largest >= count - 1 else 0
    holding, surplus = [largest] + [least] * (count - 1), total - largest - least * (count - 1)
    while surplus > 0:
        free = [i for i in range(1, count) if holding[i] < largest] or [i for i in range(1, count) if holding[i] < most]
        whole, left = sum([weights[i] for i in free]), surplus
        for i in free:
            more = min(most - holding[i], max(1, left * weights[i] // whole), surplus)
            holding[i] = holding[i] + more
            surplus = surplus - more
    return np.array(holding)


def bell_draw(key, extent, width, most, cuts=(), kind=jnp.bfloat16):
    array = width * jax.random.normal(key, extent, jnp.float32)
    if cuts:
        array = array * steps_of(key, extent, cuts, -0.22, 0.18)
    return jnp.clip(array, -most, most).astype(kind)


def setup_inputs(seed: int = 0) -> dict:
    seeds = jax.random.split(jax.random.key(seed), 8)
    parcel_props = bell_draw(seeds[0], (PROPS, PARCELS), 1.0, 6.0, ((1, 32),), jnp.float32)
    size_class = place_ends(jax.random.randint(seeds[1], (PARCELS,), 0, CLASSES), jax.random.fold_in(seeds[1], 1), 0, CLASSES - 1).astype(jnp.int32)
    dest_owner_keys = jax.random.split(jax.random.fold_in(seeds[2], 1), PARCELS // PARC_DEV)
    dest_owner_turns = jax.random.permutation(jax.random.fold_in(seeds[2], 3), PARCELS // PARC_DEV)
    dest_owner = jax.vmap(lambda own, number: routed_block(jax.random.fold_in(seeds[2], 2), own, number, PARC_DEV, DEVICES, 1, CAP, 2))(dest_owner_keys, dest_owner_turns).reshape((PARCELS, 1))
    dest_local = place_ends(jax.random.randint(seeds[3], (PARCELS,), 0, LX * LY), jax.random.fold_in(seeds[3], 1), 0, (LX * LY) - 1).astype(jnp.int32)
    class_table = jnp.clip(jnp.exp(jax.random.uniform(seeds[4], (CLASSES, PROPS), jnp.float32, math.log(0.5), math.log(2.0))), 0.5, 2.0)
    gas_density = jnp.clip(jnp.exp(math.log(2.0) - 1.3862944 * jax.random.uniform(seeds[5], (NX, NY), jnp.float32) ** steps_of(seeds[5], (NX, NY), ((0, 8), (1, 4)), -0.2, 0.2)), 0.5, 2.0)
    gas_rest = bell_draw(seeds[6], (4, NX, NY), 1.0, 6.0, ((1, 8), (2, 4)), jnp.float32)
    return dict(parcel_props=parcel_props, size_class=size_class, dest_owner=dest_owner, dest_local=dest_local, class_table=class_table, gas_density=gas_density, gas_rest=gas_rest)


def sources_of(props, classes, gas, table):
    picks = (classes[None, :] == jnp.arange(CLASSES, dtype=jnp.int32)[:, None]).astype(jnp.float32)
    coef = jnp.dot(table.T, picks, precision=lax.Precision.HIGHEST, preferred_element_type=jnp.float32)
    mass = jnp.exp(0.5 * props[0])
    density = gas[0]
    velocity = gas[1:4] / density
    theta = gas[4] / density
    slip = props[1:4] - velocity
    rate = coef[0] * jax.nn.softplus(props[4] - theta)
    evapor = mass * (1.0 - jnp.exp(-rate))
    dragged = 1.0 - jnp.exp(-coef[1] * jnp.sqrt(1.0 + lax.optimization_barrier(jnp.sum(slip * slip, axis=0))))
    moment = evapor * coef[2:5] * props[1:4] + mass * dragged * slip
    energy = evapor * (props[4] + lax.optimization_barrier(jnp.sum(coef[5:] * props[5:], axis=0)))
    return jnp.concatenate([evapor[None], moment, energy[None]], axis=0)

def smooth_field(deposit):
    padded = jnp.pad(deposit, ((0, 0), (1, 1), (1, 1)))
    beside = padded[:, 2:, 1:-1] + padded[:, :-2, 1:-1] + padded[:, 1:-1, 2:] + padded[:, 1:-1, :-2]
    return 0.4 * deposit + 0.15 * beside

def reference(parcel_props, size_class, dest_owner, dest_local, class_table, gas_density, gas_rest):
    owner = dest_owner[:, 0]
    cell_x = owner // N_GY * LX + dest_local // LY
    cell_y = owner % N_GY * LY + dest_local % LY
    flat = (cell_x * NY + cell_y).astype(jnp.int32)
    gas = jnp.concatenate([gas_density[None], gas_rest], axis=0).reshape(5, NX * NY)
    local_gas = gas[:, flat]
    source = sources_of(parcel_props, size_class, local_gas, class_table)
    deposit = jnp.zeros((5, NX * NY), jnp.float32).at[:, flat].add(source).reshape(5, NX, NY)
    smooth = smooth_field(deposit)
    return (gas_density + smooth[0], gas_rest + smooth[1:])
```

```python
import math

import jax
import jax.numpy as jnp
from jax import lax
from jax.experimental import pallas as pl
from jax.experimental.pallas import tpu as pltpu
from jax.sharding import PartitionSpec as P

F32, BF16, I32 = jnp.float32, jnp.bfloat16, jnp.int32
NT = (((1,), (1,)), ((), ()))
LANES = 256
VALUES = 8


def shift_of(n):
    assert n & (n - 1) == 0
    return n.bit_length() - 1


def split2(x):
    top = x.astype(BF16)
    return top, (x - top.astype(F32)).astype(BF16)


def hot(rows, row):
    kinds = lax.broadcasted_iota(I32, (rows, row.shape[1]), 0)
    return (kinds == row).astype(F32).astype(BF16)


def bucket_kernel(props_ref, cls_ref, own_ref, cell_ref, tab_ref, out_ref, a_ref, *, devices, cap, lw):
    n = props_ref.shape[1]
    slots = devices * cap
    his = slots // lw
    tri = (
        lax.broadcasted_iota(I32, (LANES, LANES), 0) < lax.broadcasted_iota(I32, (LANES, LANES), 1)
    ).astype(F32).astype(BF16)
    carry = (lax.broadcasted_iota(I32, (devices, 1), 0) * cap).astype(F32)
    slot = []
    for k in range(n // LANES):
        own = own_ref[:, k * LANES : (k + 1) * LANES]
        member = (lax.broadcasted_iota(I32, (devices, LANES), 0) == own).astype(F32)
        before = jnp.dot(member.astype(BF16), tri, preferred_element_type=F32)
        slot.append(jnp.sum(member * (before + carry), axis=0, keepdims=True))
        carry = carry + jnp.sum(member, axis=1, keepdims=True)
    slot = jnp.concatenate(slot, axis=1).astype(I32)
    hi = lax.shift_right_logical(slot, shift_of(lw))
    lo = slot & (lw - 1)
    table = tab_ref[...]
    col = lax.broadcasted_iota(I32, table.shape, 1)
    table = jnp.where(col > 4, table, jnp.where(col == 4, 1.0, 0.0))
    mixed = jnp.dot(
        table, props_ref[...], precision=lax.Precision.HIGHEST, preferred_element_type=F32
    )
    kinds = lax.broadcasted_iota(I32, mixed.shape, 0)
    total = jnp.sum(jnp.where(kinds == cls_ref[...], mixed, 0.0), axis=0, keepdims=True)
    vals = props_ref[0:VALUES, :]
    row = lax.broadcasted_iota(I32, vals.shape, 0)
    vals = jnp.where(row == 0, jnp.exp(0.5 * vals), vals)
    vals = jnp.where(row == 5, total, vals)
    vals = jnp.where(row == 6, cls_ref[...].astype(F32), vals)
    vals = jnp.where(row == 7, cell_ref[...].astype(F32), vals)
    top, low = split2(vals)
    pair = jnp.concatenate([top, low], axis=0)
    low_hot = hot(lw, lo)
    hi_b = jnp.broadcast_to(hi.astype(F32), (2 * VALUES, n)).astype(BF16)
    zero = jnp.zeros_like(pair)
    block = min(his, 32)
    for b in range(his // block):
        for h in range(block):
            a_ref[h * 2 * VALUES : (h + 1) * 2 * VALUES, :] = jnp.where(
                hi_b == jnp.asarray(b * block + h, BF16), pair, zero
            )
        placed = lax.dot_general(a_ref[...], low_hot, NT, preferred_element_type=F32)
        placed = placed.reshape(block, 2, VALUES, lw)
        out_ref[b * block : (b + 1) * block] = placed[:, 0] + placed[:, 1]


def owner_kernel(
    x_ref, tab_ref, rho_ref, rest_ref, dep_ref, g_ref, y_ref, a_ref, acc_ref, s_ref
):
    slab_x, slab_y = rho_ref.shape
    fold = LANES // slab_y
    xs = slab_x // fold
    classes = tab_ref.shape[0]
    for f in range(fold):
        rho = rho_ref[pl.ds(f, xs, stride=fold), :]
        for c in range(4):
            ratio = rest_ref[c, pl.ds(f, xs, stride=fold), :] / rho
            top, low = split2(ratio)
            g_ref[c * xs : (c + 1) * xs, f * slab_y : (f + 1) * slab_y] = top
            g_ref[(4 + c) * xs : (5 + c) * xs, f * slab_y : (f + 1) * slab_y] = low
    acc_ref[...] = jnp.zeros_like(acc_ref)
    half = LANES // 2
    s_ref[0] = x_ref[:, :half]
    s_ref[1] = x_ref[:, half:]
    rows = 8
    groups = x_ref.shape[0] // (rows * VALUES)
    y_shift = shift_of(LANES)

    def group(g, _):
        base = g * (rows * VALUES)
        mass, q1, q2, q3, q4, total, cls, cell = [
            jnp.concatenate(
                [s_ref[i, pl.ds(base + v, rows, stride=VALUES), :] for i in range(2)], axis=1
            )
            for v in range(VALUES)
        ]
        cell = cell.astype(I32)
        cell_x = lax.shift_right_logical(cell, y_shift)
        cell_y = cell & (LANES - 1)
        gas = [[] for _ in range(4)]
        masks = []
        for r in range(rows):
            y_hot = hot(LANES, cell_y[r : r + 1])
            y_ref[:, r * LANES : (r + 1) * LANES] = y_hot
            found = jnp.dot(g_ref[...], y_hot, preferred_element_type=F32)
            mask = lax.broadcasted_iota(I32, (xs, LANES), 0) == cell_x[r : r + 1]
            masks.append(mask)
            for c in range(4):
                both = found[c * xs : (c + 1) * xs] + found[(4 + c) * xs : (5 + c) * xs]
                gas[c].append(jnp.sum(jnp.where(mask, both, 0.0), axis=0, keepdims=True))
        v1, v2, v3, theta = [jnp.concatenate(part, axis=0) for part in gas]
        coef = []
        for j in range(5):
            picked = jnp.full(cls.shape, tab_ref[0, j], F32)
            for k in range(1, classes):
                picked = jnp.where(cls == float(k), tab_ref[k, j], picked)
            coef.append(picked)
        w1, w2, w3 = q1 - v1, q2 - v2, q3 - v3
        heat = q4 - theta
        soft = jnp.maximum(heat, 0.0) + jnp.log1p(jnp.exp(-jnp.abs(heat)))
        evapor = mass * (1.0 - jnp.exp(-(coef[0] * soft)))
        dragged = 1.0 - jnp.exp(-coef[1] * jnp.sqrt(1.0 + (w1 * w1 + w2 * w2 + w3 * w3)))
        drag = mass * dragged
        source = [
            evapor,
            evapor * coef[2] * q1 + drag * w1,
            evapor * coef[3] * q2 + drag * w2,
            evapor * coef[4] * q3 + drag * w3,
            evapor * total,
        ]
        for c in range(5):
            for r in range(rows):
                line = jnp.where(masks[r], source[c][r : r + 1], 0.0)
                top, low = split2(line)
                a_ref[c * xs : (c + 1) * xs, r * LANES : (r + 1) * LANES] = top
                a_ref[(5 + c) * xs : (6 + c) * xs, r * LANES : (r + 1) * LANES] = low
        acc_ref[...] += lax.dot_general(a_ref[...], y_ref[...], NT, preferred_element_type=F32)
        return 0

    lax.fori_loop(0, groups, group, 0)
    for c in range(5):
        both = acc_ref[c * xs : (c + 1) * xs, :] + acc_ref[(5 + c) * xs : (6 + c) * xs, :]
        for f in range(fold):
            dep_ref[c, pl.ds(f, xs, stride=fold), :] = both[:, f * slab_y : (f + 1) * slab_y]


def shifted(edge, axis, step):
    devices = lax.axis_size(axis)
    pairs = [(i, i + step) for i in range(devices) if 0 <= i + step < devices]
    return lax.ppermute(edge, axis, pairs)


def per_device(
    parcel_props, size_class, dest_owner, dest_local, class_table, gas_density, gas_rest
):
    devices = lax.axis_size("gx") * lax.axis_size("gy")
    props, parcels = parcel_props.shape
    slab_x, slab_y = gas_density.shape
    cap = max(2, 4 * parcels // devices)
    slots = devices * cap
    lw = math.gcd(cap, LANES)
    his = slots // lw
    vmem = pl.BlockSpec(memory_space=pltpu.VMEM)
    smem = pl.BlockSpec(memory_space=pltpu.SMEM)
    sent = pl.pallas_call(
        lambda *refs: bucket_kernel(*refs, devices=devices, cap=cap, lw=lw),
        out_shape=jax.ShapeDtypeStruct((his, VALUES, lw), F32),
        in_specs=[vmem] * 5,
        out_specs=vmem,
        scratch_shapes=[pltpu.VMEM((min(his, 32) * 2 * VALUES, parcels), BF16)],
        name="bucket",
    )(
        parcel_props,
        size_class.reshape(1, parcels),
        dest_owner.reshape(1, parcels),
        dest_local.reshape(1, parcels),
        class_table,
    )
    got = lax.all_to_all(sent, ("gx", "gy"), split_axis=0, concat_axis=0, tiled=True)
    if lw != LANES:
        got = got.reshape(slots // LANES, LANES // lw, VALUES, lw).transpose(0, 2, 1, 3)
    xs = slab_x * slab_y // LANES
    deposit = pl.pallas_call(
        owner_kernel,
        out_shape=jax.ShapeDtypeStruct((5, slab_x, slab_y), F32),
        in_specs=[vmem, smem, vmem, vmem],
        out_specs=vmem,
        scratch_shapes=[
            pltpu.VMEM((8 * xs, LANES), BF16),
            pltpu.VMEM((LANES, 8 * LANES), BF16),
            pltpu.VMEM((10 * xs, 8 * LANES), BF16),
            pltpu.VMEM((10 * xs, LANES), F32),
            pltpu.VMEM((2, slots // LANES * VALUES, LANES // 2), F32),
        ],
        name="owner",
    )(got.reshape(slots // LANES * VALUES, LANES), class_table, gas_density, gas_rest)
    above = shifted(deposit[:, -1:, :], "gx", 1)
    below = shifted(deposit[:, :1, :], "gx", -1)
    left = shifted(deposit[:, :, -1:], "gy", 1)
    right = shifted(deposit[:, :, :1], "gy", -1)
    tall = jnp.concatenate([above, deposit, below], axis=1)
    wide = jnp.concatenate([left, deposit, right], axis=2)
    beside = tall[:, 2:] + tall[:, :-2] + wide[:, :, 2:] + wide[:, :, :-2]
    smooth = 0.4 * deposit + 0.15 * beside
    return (gas_density + smooth[0], gas_rest + smooth[1:])


def solution(mesh):
    return jax.shard_map(
        per_device,
        mesh=mesh,
        in_specs=(
            P(None, ("gx", "gy")),
            P(("gx", "gy")),
            P(("gx", "gy"), None),
            P(("gx", "gy")),
            P(),
            P("gx", "gy"),
            P(None, "gx", "gy"),
        ),
        out_specs=(P("gx", "gy"), P(None, "gx", "gy")),
        check_vma=False,
    )
```

```python
import math

import jax
import jax.numpy as jnp
from jax import lax
from jax.experimental import pallas as pl
from jax.experimental.pallas import tpu as pltpu
from jax.sharding import PartitionSpec as P

F32, BF16, I32 = jnp.float32, jnp.bfloat16, jnp.int32
NT = (((1,), (1,)), ((), ()))
LANES = 256
VALUES = 8


def shift_of(n):
    assert n & (n - 1) == 0
    return n.bit_length() - 1


def split2(x):
    top = x.astype(BF16)
    return top, (x - top.astype(F32)).astype(BF16)


def hot(rows, row):
    kinds = lax.broadcasted_iota(I32, (rows, row.shape[1]), 0)
    return (kinds == row).astype(F32).astype(BF16)


def bucket_kernel(props_ref, cls_ref, own_ref, cell_ref, tab_ref, out_ref, a_ref, *, devices, cap, lw):
    n = props_ref.shape[1]
    slots = devices * cap
    his = slots // lw
    tri = (
        lax.broadcasted_iota(I32, (LANES, LANES), 0) < lax.broadcasted_iota(I32, (LANES, LANES), 1)
    ).astype(F32).astype(BF16)
    carry = (lax.broadcasted_iota(I32, (devices, 1), 0) * cap).astype(F32)
    slot = []
    for k in range(n // LANES):
        own = own_ref[:, k * LANES : (k + 1) * LANES]
        member = (lax.broadcasted_iota(I32, (devices, LANES), 0) == own).astype(F32)
        before = jnp.dot(member.astype(BF16), tri, preferred_element_type=F32)
        slot.append(jnp.sum(member * (before + carry), axis=0, keepdims=True))
        carry = carry + jnp.sum(member, axis=1, keepdims=True)
    slot = jnp.concatenate(slot, axis=1).astype(I32)
    hi = lax.shift_right_logical(slot, shift_of(lw))
    lo = slot & (lw - 1)
    table = tab_ref[...]
    col = lax.broadcasted_iota(I32, table.shape, 1)
    table = jnp.where(col > 4, table, jnp.where(col == 4, 1.0, 0.0))
    mixed = jnp.dot(
        table, props_ref[...], precision=lax.Precision.HIGHEST, preferred_element_type=F32
    )
    kinds = lax.broadcasted_iota(I32, mixed.shape, 0)
    total = jnp.sum(jnp.where(kinds == cls_ref[...], mixed, 0.0), axis=0, keepdims=True)
    vals = props_ref[0:VALUES, :]
    row = lax.broadcasted_iota(I32, vals.shape, 0)
    vals = jnp.where(row == 0, jnp.exp(0.5 * vals), vals)
    vals = jnp.where(row == 5, total, vals)
    vals = jnp.where(row == 6, cls_ref[...].astype(F32), vals)
    vals = jnp.where(row == 7, cell_ref[...].astype(F32), vals)
    top, low = split2(vals)
    pair = jnp.concatenate([top, low], axis=0)
    low_hot = hot(lw, lo)
    hi_b = jnp.broadcast_to(hi.astype(F32), (2 * VALUES, n)).astype(BF16)
    zero = jnp.zeros_like(pair)
    block = min(his, 32)
    for b in range(his // block):
        for h in range(block):
            a_ref[h * 2 * VALUES : (h + 1) * 2 * VALUES, :] = jnp.where(
                hi_b == jnp.asarray(b * block + h, BF16), pair, zero
            )
        placed = lax.dot_general(a_ref[...], low_hot, NT, preferred_element_type=F32)
        placed = placed.reshape(block, 2, VALUES, lw)
        out_ref[b * block : (b + 1) * block] = placed[:, 0] + placed[:, 1]


def owner_kernel(
    x_ref, tab_ref, rho_ref, rest_ref, dep_ref, g_ref, y_ref, a_ref, acc_ref, s_ref
):
    slab_x, slab_y = rho_ref.shape
    fold = LANES // slab_y
    xs = slab_x // fold
    classes = tab_ref.shape[0]
    for f in range(fold):
        rho = rho_ref[pl.ds(f, xs, stride=fold), :]
        for c in range(4):
            ratio = rest_ref[c, pl.ds(f, xs, stride=fold), :] / rho
            top, low = split2(ratio)
            g_ref[c * xs : (c + 1) * xs, f * slab_y : (f + 1) * slab_y] = top
            g_ref[(4 + c) * xs : (5 + c) * xs, f * slab_y : (f + 1) * slab_y] = low
    acc_ref[...] = jnp.zeros_like(acc_ref)
    half = LANES // 2
    s_ref[0] = x_ref[:, :half]
    s_ref[1] = x_ref[:, half:]
    rows = 8
    groups = x_ref.shape[0] // (rows * VALUES)
    y_shift = shift_of(LANES)

    def group(g, _):
        base = g * (rows * VALUES)
        mass, q1, q2, q3, q4, total, cls, cell = [
            jnp.concatenate(
                [s_ref[i, pl.ds(base + v, rows, stride=VALUES), :] for i in range(2)], axis=1
            )
            for v in range(VALUES)
        ]
        cell = cell.astype(I32)
        cell_x = lax.shift_right_logical(cell, y_shift)
        cell_y = cell & (LANES - 1)
        gas = [[] for _ in range(4)]
        masks = []
        for r in range(rows):
            y_hot = hot(LANES, cell_y[r : r + 1])
            y_ref[:, r * LANES : (r + 1) * LANES] = y_hot
            found = jnp.dot(g_ref[...], y_hot, preferred_element_type=F32)
            mask = lax.broadcasted_iota(I32, (xs, LANES), 0) == cell_x[r : r + 1]
            masks.append(mask)
            for c in range(4):
                both = found[c * xs : (c + 1) * xs] + found[(4 + c) * xs : (5 + c) * xs]
                gas[c].append(jnp.sum(jnp.where(mask, both, 0.0), axis=0, keepdims=True))
        v1, v2, v3, theta = [jnp.concatenate(part, axis=0) for part in gas]
        coef = []
        for j in range(5):
            picked = jnp.full(cls.shape, tab_ref[0, j], F32)
            for k in range(1, classes):
                picked = jnp.where(cls == float(k), tab_ref[k, j], picked)
            coef.append(picked)
        w1, w2, w3 = q1 - v1, q2 - v2, q3 - v3
        heat = q4 - theta
        soft = jnp.maximum(heat, 0.0) + jnp.log1p(jnp.exp(-jnp.abs(heat)))
        evapor = mass * (1.0 - jnp.exp(-(coef[0] * soft)))
        dragged = 1.0 - jnp.exp(-coef[1] * jnp.sqrt(1.0 + (w1 * w1 + w2 * w2 + w3 * w3)))
        drag = mass * dragged
        source = [
            evapor,
            evapor * coef[2] * q1 + drag * w1,
            evapor * coef[3] * q2 + drag * w2,
            evapor * coef[4] * q3 + drag * w3,
            evapor * total,
        ]
        for c in range(5):
            for r in range(rows):
                line = jnp.where(masks[r], source[c][r : r + 1], 0.0)
                top, low = split2(line)
                a_ref[c * xs : (c + 1) * xs, r * LANES : (r + 1) * LANES] = top
                a_ref[(5 + c) * xs : (6 + c) * xs, r * LANES : (r + 1) * LANES] = low
        acc_ref[...] += lax.dot_general(a_ref[...], y_ref[...], NT, preferred_element_type=F32)
        return 0

    lax.fori_loop(0, groups, group, 0)
    for c in range(5):
        both = acc_ref[c * xs : (c + 1) * xs, :] + acc_ref[(5 + c) * xs : (6 + c) * xs, :]
        for f in range(fold):
            dep_ref[c, pl.ds(f, xs, stride=fold), :] = both[:, f * slab_y : (f + 1) * slab_y]


def exchanged(first, last, axis):
    devices = lax.axis_size(axis)
    even = lax.axis_index(axis) % 2 == 0
    got = []
    for start in (0, 1):
        pairs = [(i, i + 1) for i in range(start, devices - 1, 2)]
        pairs = pairs + [(j, i) for i, j in pairs]
        lower = even if start == 0 else jnp.logical_not(even)
        got.append(lax.ppermute(jnp.where(lower, last, first), axis, pairs))
    return jnp.where(even, got[1], got[0]), jnp.where(even, got[0], got[1])


def per_device(
    parcel_props, size_class, dest_owner, dest_local, class_table, gas_density, gas_rest
):
    devices = lax.axis_size("gx") * lax.axis_size("gy")
    props, parcels = parcel_props.shape
    slab_x, slab_y = gas_density.shape
    cap = max(2, 4 * parcels // devices)
    slots = devices * cap
    lw = math.gcd(cap, LANES)
    his = slots // lw
    vmem = pl.BlockSpec(memory_space=pltpu.VMEM)
    smem = pl.BlockSpec(memory_space=pltpu.SMEM)
    sent = pl.pallas_call(
        lambda *refs: bucket_kernel(*refs, devices=devices, cap=cap, lw=lw),
        out_shape=jax.ShapeDtypeStruct((his, VALUES, lw), F32),
        in_specs=[vmem] * 5,
        out_specs=vmem,
        scratch_shapes=[pltpu.VMEM((min(his, 32) * 2 * VALUES, parcels), BF16)],
        name="bucket",
    )(
        parcel_props,
        size_class.reshape(1, parcels),
        dest_owner.reshape(1, parcels),
        dest_local.reshape(1, parcels),
        class_table,
    )
    got = lax.all_to_all(sent, ("gx", "gy"), split_axis=0, concat_axis=0, tiled=True)
    if lw != LANES:
        got = got.reshape(slots // LANES, LANES // lw, VALUES, lw).transpose(0, 2, 1, 3)
    xs = slab_x * slab_y // LANES
    deposit = pl.pallas_call(
        owner_kernel,
        out_shape=jax.ShapeDtypeStruct((5, slab_x, slab_y), F32),
        in_specs=[vmem, smem, vmem, vmem],
        out_specs=vmem,
        scratch_shapes=[
            pltpu.VMEM((8 * xs, LANES), BF16),
            pltpu.VMEM((LANES, 8 * LANES), BF16),
            pltpu.VMEM((10 * xs, 8 * LANES), BF16),
            pltpu.VMEM((10 * xs, LANES), F32),
            pltpu.VMEM((2, slots // LANES * VALUES, LANES // 2), F32),
        ],
        name="owner",
    )(got.reshape(slots // LANES * VALUES, LANES), class_table, gas_density, gas_rest)
    left, right = exchanged(deposit[:, :, :1], deposit[:, :, -1:], "gy")
    above, below = exchanged(deposit[:, :1, :], deposit[:, -1:, :], "gx")
    tall = jnp.concatenate([above, deposit, below], axis=1)
    wide = jnp.concatenate([left, deposit, right], axis=2)
    beside = tall[:, 2:] + tall[:, :-2] + wide[:, :, 2:] + wide[:, :, :-2]
    smooth = 0.4 * deposit + 0.15 * beside
    return (gas_density + smooth[0], gas_rest + smooth[1:])


def solution(mesh):
    return jax.shard_map(
        per_device,
        mesh=mesh,
        in_specs=(
            P(None, ("gx", "gy")),
            P(("gx", "gy")),
            P(("gx", "gy"), None),
            P(("gx", "gy")),
            P(),
            P("gx", "gy"),
            P(None, "gx", "gy"),
        ),
        out_specs=(P("gx", "gy"), P(None, "gx", "gy")),
        check_vma=False,
    )
```

```python
import math

import jax
import jax.numpy as jnp
from jax import lax
from jax.experimental import pallas as pl
from jax.experimental.pallas import tpu as pltpu
from jax.sharding import PartitionSpec as P

F32, BF16, I32 = jnp.float32, jnp.bfloat16, jnp.int32
NT = (((1,), (1,)), ((), ()))
LANES = 256
VALUES = 8


def shift_of(n):
    assert n & (n - 1) == 0
    return n.bit_length() - 1


def split2(x):
    top = x.astype(BF16)
    return top, (x - top.astype(F32)).astype(BF16)


def hot(rows, row):
    kinds = lax.broadcasted_iota(I32, (rows, row.shape[1]), 0)
    return (kinds == row).astype(F32).astype(BF16)


def bucket_kernel(props_ref, cls_ref, own_ref, cell_ref, tab_ref, out_ref, a_ref, *, devices, cap, lw):
    n = props_ref.shape[1]
    slots = devices * cap
    his = slots // lw
    tri = (
        lax.broadcasted_iota(I32, (LANES, LANES), 0) < lax.broadcasted_iota(I32, (LANES, LANES), 1)
    ).astype(F32).astype(BF16)
    carry = (lax.broadcasted_iota(I32, (devices, 1), 0) * cap).astype(F32)
    slot = []
    for k in range(n // LANES):
        own = own_ref[:, k * LANES : (k + 1) * LANES]
        member = (lax.broadcasted_iota(I32, (devices, LANES), 0) == own).astype(F32)
        before = jnp.dot(member.astype(BF16), tri, preferred_element_type=F32)
        slot.append(jnp.sum(member * (before + carry), axis=0, keepdims=True))
        carry = carry + jnp.sum(member, axis=1, keepdims=True)
    slot = jnp.concatenate(slot, axis=1).astype(I32)
    hi = lax.shift_right_logical(slot, shift_of(lw))
    lo = slot & (lw - 1)
    table = tab_ref[...]
    col = lax.broadcasted_iota(I32, table.shape, 1)
    table = jnp.where(col > 4, table, jnp.where(col == 4, 1.0, 0.0))
    mixed = jnp.dot(
        table, props_ref[...], precision=lax.Precision.HIGHEST, preferred_element_type=F32
    )
    kinds = lax.broadcasted_iota(I32, mixed.shape, 0)
    total = jnp.sum(jnp.where(kinds == cls_ref[...], mixed, 0.0), axis=0, keepdims=True)
    vals = props_ref[0:VALUES, :]
    row = lax.broadcasted_iota(I32, vals.shape, 0)
    vals = jnp.where(row == 0, jnp.exp(0.5 * vals), vals)
    vals = jnp.where(row == 5, total, vals)
    vals = jnp.where(row == 6, cls_ref[...].astype(F32), vals)
    vals = jnp.where(row == 7, cell_ref[...].astype(F32), vals)
    top, low = split2(vals)
    pair = jnp.concatenate([top, low], axis=0)
    low_hot = hot(lw, lo)
    hi_b = jnp.broadcast_to(hi.astype(F32), (2 * VALUES, n)).astype(BF16)
    zero = jnp.zeros_like(pair)
    block = min(his, 32)
    for b in range(his // block):
        for h in range(block):
            a_ref[h * 2 * VALUES : (h + 1) * 2 * VALUES, :] = jnp.where(
                hi_b == jnp.asarray(b * block + h, BF16), pair, zero
            )
        placed = lax.dot_general(a_ref[...], low_hot, NT, preferred_element_type=F32)
        placed = placed.reshape(block, 2, VALUES, lw)
        out_ref[b * block : (b + 1) * block] = placed[:, 0] + placed[:, 1]


def owner_kernel(
    x_ref, tab_ref, rho_ref, rest_ref, dep_ref, g_ref, y_ref, a_ref, acc_ref, s_ref
):
    slab_x, slab_y = rho_ref.shape
    fold = LANES // slab_y
    xs = slab_x // fold
    classes = tab_ref.shape[0]
    for f in range(fold):
        rho = rho_ref[pl.ds(f, xs, stride=fold), :]
        for c in range(4):
            ratio = rest_ref[c, pl.ds(f, xs, stride=fold), :] / rho
            top, low = split2(ratio)
            g_ref[c * xs : (c + 1) * xs, f * slab_y : (f + 1) * slab_y] = top
            g_ref[(4 + c) * xs : (5 + c) * xs, f * slab_y : (f + 1) * slab_y] = low
    acc_ref[...] = jnp.zeros_like(acc_ref)
    half = LANES // 2
    s_ref[0] = x_ref[:, :half]
    s_ref[1] = x_ref[:, half:]
    rows = 8
    groups = x_ref.shape[0] // (rows * VALUES)
    y_shift = shift_of(LANES)

    def group(g, b):
        base = g * (rows * VALUES)
        mass, q1, q2, q3, q4, total, cls, cell = [
            jnp.concatenate(
                [s_ref[i, pl.ds(base + v, rows, stride=VALUES), :] for i in range(2)], axis=1
            )
            for v in range(VALUES)
        ]
        cell = cell.astype(I32)
        cell_x = lax.shift_right_logical(cell, y_shift)
        cell_y = cell & (LANES - 1)
        gas = [[] for _ in range(4)]
        masks = []
        for r in range(rows):
            y_hot = hot(LANES, cell_y[r : r + 1])
            y_ref[b, :, r * LANES : (r + 1) * LANES] = y_hot
            found = jnp.dot(g_ref[...], y_hot, preferred_element_type=F32)
            mask = lax.broadcasted_iota(I32, (xs, LANES), 0) == cell_x[r : r + 1]
            masks.append(mask)
            for c in range(4):
                both = found[c * xs : (c + 1) * xs] + found[(4 + c) * xs : (5 + c) * xs]
                gas[c].append(jnp.sum(jnp.where(mask, both, 0.0), axis=0, keepdims=True))
        v1, v2, v3, theta = [jnp.concatenate(part, axis=0) for part in gas]
        coef = []
        for j in range(5):
            picked = jnp.full(cls.shape, tab_ref[0, j], F32)
            for k in range(1, classes):
                picked = jnp.where(cls == float(k), tab_ref[k, j], picked)
            coef.append(picked)
        w1, w2, w3 = q1 - v1, q2 - v2, q3 - v3
        heat = q4 - theta
        soft = jnp.maximum(heat, 0.0) + jnp.log1p(jnp.exp(-jnp.abs(heat)))
        evapor = mass * (1.0 - jnp.exp(-(coef[0] * soft)))
        dragged = 1.0 - jnp.exp(-coef[1] * jnp.sqrt(1.0 + (w1 * w1 + w2 * w2 + w3 * w3)))
        drag = mass * dragged
        source = [
            evapor,
            evapor * coef[2] * q1 + drag * w1,
            evapor * coef[3] * q2 + drag * w2,
            evapor * coef[4] * q3 + drag * w3,
            evapor * total,
        ]
        for c in range(5):
            for r in range(rows):
                line = jnp.where(masks[r], source[c][r : r + 1], 0.0)
                top, low = split2(line)
                a_ref[b, c * xs : (c + 1) * xs, r * LANES : (r + 1) * LANES] = top
                a_ref[b, (5 + c) * xs : (6 + c) * xs, r * LANES : (r + 1) * LANES] = low
        acc_ref[...] += lax.dot_general(a_ref[b], y_ref[b], NT, preferred_element_type=F32)

    def couple(i, _):
        group(2 * i, 0)
        group(2 * i + 1, 1)
        return 0

    assert groups % 2 == 0
    lax.fori_loop(0, groups // 2, couple, 0)
    for c in range(5):
        both = acc_ref[c * xs : (c + 1) * xs, :] + acc_ref[(5 + c) * xs : (6 + c) * xs, :]
        for f in range(fold):
            dep_ref[c, pl.ds(f, xs, stride=fold), :] = both[:, f * slab_y : (f + 1) * slab_y]


def exchanged(first, last, axis):
    devices = lax.axis_size(axis)
    even = lax.axis_index(axis) % 2 == 0
    got = []
    for start in (0, 1):
        pairs = [(i, i + 1) for i in range(start, devices - 1, 2)]
        pairs = pairs + [(j, i) for i, j in pairs]
        lower = even if start == 0 else jnp.logical_not(even)
        got.append(lax.ppermute(jnp.where(lower, last, first), axis, pairs))
    return jnp.where(even, got[1], got[0]), jnp.where(even, got[0], got[1])


def per_device(
    parcel_props, size_class, dest_owner, dest_local, class_table, gas_density, gas_rest
):
    devices = lax.axis_size("gx") * lax.axis_size("gy")
    props, parcels = parcel_props.shape
    slab_x, slab_y = gas_density.shape
    cap = max(2, 4 * parcels // devices)
    slots = devices * cap
    lw = math.gcd(cap, LANES)
    his = slots // lw
    vmem = pl.BlockSpec(memory_space=pltpu.VMEM)
    smem = pl.BlockSpec(memory_space=pltpu.SMEM)
    sent = pl.pallas_call(
        lambda *refs: bucket_kernel(*refs, devices=devices, cap=cap, lw=lw),
        out_shape=jax.ShapeDtypeStruct((his, VALUES, lw), F32),
        in_specs=[vmem] * 5,
        out_specs=vmem,
        scratch_shapes=[pltpu.VMEM((min(his, 32) * 2 * VALUES, parcels), BF16)],
        name="bucket",
    )(
        parcel_props,
        size_class.reshape(1, parcels),
        dest_owner.reshape(1, parcels),
        dest_local.reshape(1, parcels),
        class_table,
    )
    got = lax.all_to_all(sent, ("gx", "gy"), split_axis=0, concat_axis=0, tiled=True)
    if lw != LANES:
        got = got.reshape(slots // LANES, LANES // lw, VALUES, lw).transpose(0, 2, 1, 3)
    xs = slab_x * slab_y // LANES
    deposit = pl.pallas_call(
        owner_kernel,
        out_shape=jax.ShapeDtypeStruct((5, slab_x, slab_y), F32),
        in_specs=[vmem, smem, vmem, vmem],
        out_specs=vmem,
        scratch_shapes=[
            pltpu.VMEM((8 * xs, LANES), BF16),
            pltpu.VMEM((2, LANES, 8 * LANES), BF16),
            pltpu.VMEM((2, 10 * xs, 8 * LANES), BF16),
            pltpu.VMEM((10 * xs, LANES), F32),
            pltpu.VMEM((2, slots // LANES * VALUES, LANES // 2), F32),
        ],
        name="owner",
    )(got.reshape(slots // LANES * VALUES, LANES), class_table, gas_density, gas_rest)
    left, right = exchanged(deposit[:, :, :1], deposit[:, :, -1:], "gy")
    above, below = exchanged(deposit[:, :1, :], deposit[:, -1:, :], "gx")
    tall = jnp.concatenate([above, deposit, below], axis=1)
    wide = jnp.concatenate([left, deposit, right], axis=2)
    beside = tall[:, 2:] + tall[:, :-2] + wide[:, :, 2:] + wide[:, :, :-2]
    smooth = 0.4 * deposit + 0.15 * beside
    return (gas_density + smooth[0], gas_rest + smooth[1:])


def solution(mesh):
    return jax.shard_map(
        per_device,
        mesh=mesh,
        in_specs=(
            P(None, ("gx", "gy")),
            P(("gx", "gy")),
            P(("gx", "gy"), None),
            P(("gx", "gy")),
            P(),
            P("gx", "gy"),
            P(None, "gx", "gy"),
        ),
        out_specs=(P("gx", "gy"), P(None, "gx", "gy")),
        check_vma=False,
    )
```
